128 devices in a mesh: dp: 1, etp: 64 (over z, y, x), ep: 2 (over core).
Axes of the slice: x: 4, y: 4, z: 4, core: 2. Of those that a mesh axis runs over, the one named last changes fastest.
Arguments:
- hidden: bfloat16 [8192, 1536], P(('dp', 'ep'))
- expert_ids: int32 [8192, 8], P(('dp', 'ep'))
- gate_wts: float32 [8192, 8], P(('dp', 'ep'))
- slot_pos: int32 [8192, 8], P(('dp', 'ep'))
- w_gate: bfloat16 [40, 1536, 512], P('ep', None, 'etp')
- w_up: bfloat16 [40, 1536, 512], P('ep', None, 'etp')
- w_down: bfloat16 [40, 512, 1536], P('ep', 'etp')
Outputs:
- output: bfloat16 [8192, 1536], P(('dp', 'ep'))
All inputs are finite; a program needn't handle non-finite values.
Results may differ from the reference program's by a relative error of at most 0.001.
Values are sent between devices in bfloat16 or wider.
A program may use at most 1 GiB of HBM per device.

```python
import jax
import jax.numpy as jnp
from jax import lax

D_MODEL = 1536
D_FF = 512
EXPERTS = 40
TOP_K = 8
TOK_DEV = 4096
GROUP = 2
LOCAL_CAP = 1024

TOKENS = TOK_DEV * GROUP
CAPACITY = LOCAL_CAP * GROUP


def rank_in_expert(flat_ids, priority):
    n_choices = flat_ids.shape[0]
    sort_order = jnp.argsort(flat_ids * n_choices + priority)
    sorted_ids = flat_ids[sort_order]
    counts = jnp.bincount(flat_ids, length=EXPERTS)
    starts = jnp.cumsum(counts) - counts
    sorted_rank = jnp.arange(n_choices) - starts[sorted_ids]
    return jnp.zeros((n_choices,), jnp.int32).at[sort_order].set(sorted_rank.astype(jnp.int32))


def draw_routing(route_key):
    key_hot, key_rows, key_bias, key_score, key_prio = jax.random.split(route_key, 5)
    hot_expert = jax.random.randint(key_hot, (GROUP,), 0, EXPERTS)
    row_perm = jax.vmap(lambda sub_key: jax.random.permutation(sub_key, TOK_DEV))(jax.random.split(key_rows, GROUP))
    forced = row_perm < LOCAL_CAP
    expert_bias = jax.random.randint(key_bias, (EXPERTS,), 0, 2 ** 19)
    scores = jax.random.randint(key_score, (GROUP, TOK_DEV, EXPERTS), 0, 2 ** 20) + expert_bias
    expert_range = jnp.arange(EXPERTS)
    is_hot = forced[:, :, None] & (expert_range[None, None, :] == hot_expert[:, None, None])
    scores = jnp.where(is_hot, 2 ** 21, scores)
    top_scores, expert_ids = lax.top_k(scores * EXPERTS + expert_range, TOP_K)
    priority = jax.vmap(lambda sub_key: jax.random.permutation(sub_key, TOK_DEV * TOP_K))(jax.random.split(key_prio, GROUP))
    local_rank = jax.vmap(rank_in_expert)(expert_ids.reshape(GROUP, TOK_DEV * TOP_K), priority)
    block_base = (jnp.arange(GROUP) * LOCAL_CAP)[:, None]
    slot_pos = jnp.where(local_rank < LOCAL_CAP, block_base + local_rank, -1)
    return expert_ids.reshape(TOKENS, TOP_K).astype(jnp.int32), slot_pos.reshape(TOKENS, TOP_K).astype(jnp.int32)


def setup_inputs(seed: int = 0, part: int = 0) -> dict:
    base_key = jax.random.key(seed)
    part_key = jax.random.fold_in(base_key, part)
    key_hidden, key_route, key_gate = jax.random.split(part_key, 3)
    key_w_gate, key_w_up, key_w_down = jax.random.split(jax.random.key(seed + 1), 3)
    hidden = jax.random.normal(key_hidden, (TOKENS, D_MODEL), jnp.float32).astype(jnp.bfloat16)
    expert_ids, slot_pos = draw_routing(key_route)
    logits = jax.random.normal(key_gate, (TOKENS, TOP_K), jnp.float32)
    gate_wts = jax.nn.softmax(logits, axis=-1)
    w_gate = (jax.random.normal(key_w_gate, (EXPERTS, D_MODEL, D_FF), jnp.float32) * D_MODEL ** -0.5).astype(jnp.bfloat16)
    w_up = (jax.random.normal(key_w_up, (EXPERTS, D_MODEL, D_FF), jnp.float32) * D_MODEL ** -0.5).astype(jnp.bfloat16)
    w_down = (jax.random.normal(key_w_down, (EXPERTS, D_FF, D_MODEL), jnp.float32) * D_FF ** -0.5).astype(jnp.bfloat16)
    return dict(hidden=hidden, expert_ids=expert_ids, gate_wts=gate_wts, slot_pos=slot_pos, w_gate=w_gate, w_up=w_up, w_down=w_down)


def reference(hidden, expert_ids, gate_wts, slot_pos, w_gate, w_up, w_down):
    flat_pos = slot_pos.reshape(-1)
    slot_index = jnp.where(flat_pos >= 0, expert_ids.reshape(-1) * CAPACITY + flat_pos, EXPERTS * CAPACITY)
    token_index = jnp.broadcast_to(jnp.arange(TOKENS, dtype=jnp.int32)[:, None], (TOKENS, TOP_K)).reshape(-1)
    slot_token = jnp.full((EXPERTS * CAPACITY,), TOKENS, jnp.int32).at[slot_index].set(token_index, mode='drop')
    slot_gate = jnp.zeros((EXPERTS * CAPACITY,), jnp.float32).at[slot_index].set(gate_wts.reshape(-1), mode='drop')

    def expert_step(running, operands):
        tok_ids, gate_col, gate_mat, up_mat, down_mat = operands
        buffer = jnp.take(hidden, tok_ids, axis=0, mode='fill', fill_value=0)
        h_gate = jnp.dot(buffer, gate_mat, preferred_element_type=jnp.float32)
        h_up = jnp.dot(buffer, up_mat, preferred_element_type=jnp.float32)
        hidden_act = (jax.nn.silu(h_gate) * h_up).astype(jnp.bfloat16)
        expert_out = jnp.dot(hidden_act, down_mat, preferred_element_type=jnp.float32)
        running = running + jax.ops.segment_sum(expert_out * gate_col[:, None], tok_ids, num_segments=TOKENS)
        return running, None

    start_sum = jnp.zeros((TOKENS, D_MODEL), jnp.float32)
    total_out, unused = lax.scan(expert_step, start_sum, (slot_token.reshape(EXPERTS, CAPACITY), slot_gate.reshape(EXPERTS, CAPACITY), w_gate, w_up, w_down))
    return total_out.astype(jnp.bfloat16)
```

```python
import jax
import jax.numpy as jnp
from jax import lax
from jax.sharding import PartitionSpec as P


def split3(a):
    hi = lax.reduce_precision(a, 8, 7)
    rest = a - hi
    mid = lax.reduce_precision(rest, 8, 7)
    low = rest - mid
    return [v.astype(jnp.bfloat16) for v in (hi, mid, low)]


def solution(mesh):
    row_spec = P(('dp', 'ep'), None)
    col_spec = P('ep', None, 'etp')
    in_specs = (row_spec, row_spec, row_spec, row_spec, col_spec, col_spec, P('ep', 'etp', None))

    def device_step(hidden, expert_ids, gate_wts, slot_pos, w_gate, w_up, w_down):
        rows, d_model = hidden.shape
        top_k = expert_ids.shape[1]
        width = w_gate.shape[2]
        w_gate = lax.all_gather(w_gate, 'ep', axis=0, tiled=True)
        w_up = lax.all_gather(w_up, 'ep', axis=0, tiled=True)
        w_down = lax.all_gather(w_down, 'ep', axis=0, tiled=True)
        experts = w_gate.shape[0]
        cols = experts * width
        wg = w_gate.transpose(1, 0, 2).reshape(d_model, cols)
        wu = w_up.transpose(1, 0, 2).reshape(d_model, cols)
        wd = w_down.reshape(cols, d_model)
        kept = slot_pos >= 0
        top = jnp.max(jnp.where(kept, gate_wts, 0.0), axis=1, keepdims=True)
        top = jnp.where(top > 0, top, 1.0)
        rel = gate_wts / top
        col_expert = jnp.arange(cols, dtype=jnp.int32) // width
        gate = jnp.zeros((rows, cols), jnp.float32)
        for j in range(top_k):
            hit = (expert_ids[:, j:j + 1] == col_expert[None, :]) & kept[:, j:j + 1]
            gate = jnp.where(hit, rel[:, j:j + 1], gate)
        h_gate = jnp.dot(hidden, wg, preferred_element_type=jnp.float32)
        h_up = jnp.dot(hidden, wu, preferred_element_type=jnp.float32)
        act = lax.reduce_precision(jax.nn.silu(h_gate) * h_up, 8, 7)
        scaled = jnp.where(gate > 0, act * gate, 0.0)
        parts = jnp.concatenate(split3(scaled), axis=1)
        part_sum = jnp.dot(parts, jnp.concatenate([wd] * 3, axis=0), preferred_element_type=jnp.float32)
        own = lax.psum_scatter(part_sum, 'etp', scatter_dimension=0, tiled=True)
        n_own = own.shape[0]
        own_top = lax.dynamic_slice_in_dim(top, lax.axis_index('etp') * n_own, n_own, 0)
        own = (own * own_top).astype(jnp.bfloat16)
        return lax.all_gather(own, 'etp', axis=0, tiled=True)

    return jax.shard_map(device_step, mesh=mesh, in_specs=in_specs, out_specs=row_spec, check_vma=False)
```

```python
import functools

import jax
import jax.numpy as jnp
from jax import lax
from jax.experimental import pallas as pl
from jax.experimental.pallas import tpu as pltpu
from jax.sharding import PartitionSpec as P

MESH = pl.DeviceIdType.MESH
SIDE = 4


def split3(a):
    hi = lax.reduce_precision(a, 8, 7)
    rest = a - hi
    mid = lax.reduce_precision(rest, 8, 7)
    low = rest - mid
    return [v.astype(jnp.bfloat16) for v in (hi, mid, low)]


def coords():
    chip = lax.axis_index('etp')
    return chip // (SIDE * SIDE), (chip // SIDE) % SIDE, chip % SIDE


def chip_id(z, y, x):
    return {'etp': ((z % SIDE) * SIDE + y % SIDE) * SIDE + x % SIDE}


def greet(partners):
    barrier = pltpu.get_barrier_semaphore()
    for device_id in partners:
        pl.semaphore_signal(barrier, inc=1, device_id=device_id, device_id_type=MESH)
    pl.semaphore_wait(barrier, len(partners))


def push(src, dst, sems, n, device_id):
    send_sem, recv_sem = sems
    copy = pltpu.make_async_remote_copy(src_ref=src, dst_ref=dst, send_sem=send_sem.at[n], recv_sem=recv_sem.at[n],
                                        device_id=device_id, device_id_type=MESH)
    copy.start()
    return copy


def weight_kernel(w_ref, out_ref, ring_send, ring_recv, core_send, core_recv, own_sem):
    z, y, x = coords()
    core = lax.axis_index('ep')
    other = {'ep': 1 - core}
    rows = w_ref.shape[1] // 2
    half = w_ref.shape[2] // 2
    rings = (ring_send, ring_recv)
    cores = (core_send, core_recv)
    right = (chip_id(z, y, x + 1), chip_id(z, y + 1, x))
    left = (chip_id(z, y, x + 3), chip_id(z, y + 3, x))
    place = (x, y)
    greet(list(right) + list(left) + [other])

    def src(d, h):
        return w_ref.at[:, pl.ds(d * rows, rows), pl.ds(h * half, half)]

    def box(d, i, h, c):
        return out_ref.at[:, d, i % SIDE, c, :, pl.ds(h * half, half)]

    flights = []
    firsts = []
    for d in range(2):
        me = place[d]
        firsts.append((push(src(d, 0), box(d, me, 0, core), rings, 6 * d, right[d]),
                       push(src(d, 1), box(d, me, 1, core), rings, 6 * d + 1, left[d])))
    seconds = []
    for d in range(2):
        me = place[d]
        seconds.append((push(src(d, 1), box(d, me, 1, core), rings, 6 * d + 2, right[d]),
                        push(src(d, 0), box(d, me, 0, core), rings, 6 * d + 3, left[d])))
        for h in range(2):
            flights.append(push(src(d, h), box(d, me, h, core), cores, 8 * d + h, other))
    owns = []
    for d in range(2):
        own = pltpu.make_async_copy(w_ref.at[:, pl.ds(d * rows, rows), :], out_ref.at[:, d, place[d], core], own_sem.at[d])
        own.start()
        owns.append(own)
    thirds = []
    for d in range(2):
        me = place[d]
        from_left, from_right = box(d, me + 3, 0, core), box(d, me + 1, 1, core)
        firsts[d][0].wait_recv()
        one = push(from_left, from_left, rings, 6 * d + 4, right[d])
        flights.append(push(from_left, from_left, cores, 8 * d + 2, other))
        firsts[d][1].wait_recv()
        two = push(from_right, from_right, rings, 6 * d + 5, left[d])
        flights.append(push(from_right, from_right, cores, 8 * d + 3, other))
        thirds.append((one, two))
    for d in range(2):
        me = place[d]
        for n, (copy, i, h) in enumerate(((seconds[d][0], me + 3, 1), (seconds[d][1], me + 1, 0),
                                          (thirds[d][0], me + 2, 0), (thirds[d][1], me + 2, 1))):
            copy.wait_recv()
            flights.append(push(box(d, i, h, core), box(d, i, h, core), cores, 8 * d + 4 + n, other))
    for copy in flights:
        copy.wait_recv()
    for pair in firsts + seconds + thirds:
        for copy in pair:
            copy.wait_send()
    for copy in flights:
        copy.wait_send()
    for own in owns:
        own.wait()


def gather_weights(weights):
    mats, rows, depth = weights.shape
    return pl.pallas_call(
        weight_kernel,
        out_shape=jax.ShapeDtypeStruct((mats, 2, SIDE, 2, rows // 2, depth), weights.dtype),
        in_specs=[pl.BlockSpec(memory_space=pltpu.VMEM)],
        out_specs=pl.BlockSpec(memory_space=pl.ANY),
        scratch_shapes=[pltpu.SemaphoreType.DMA((12,)), pltpu.SemaphoreType.DMA((12,)),
                        pltpu.SemaphoreType.DMA((16,)), pltpu.SemaphoreType.DMA((16,)),
                        pltpu.SemaphoreType.DMA((2,))],
        compiler_params=pltpu.CompilerParams(collective_id=0, has_side_effects=True),
        name='gather_weights',
    )(weights)


def combine_kernel(part_a, part_b, top_ref, out_ref, opp1, fin1, sum1, opp2, fin2, gath,
                   rs_send, rs_recv, ag_send, ag_recv, out_sem):
    z, y, x = coords()
    width = part_a.shape[3]
    n_rows = part_a.shape[2]
    third = out_ref.shape[4] // 3
    ups = {'z': chip_id(z + 1, y, x), 'y': chip_id(z, y + 1, x), 'x': chip_id(z, y, x + 1), 'd': chip_id(z, y + 3, x + 1)}
    downs = {'z': chip_id(z + 3, y, x), 'y': chip_id(z, y + 3, x), 'x': chip_id(z, y, x + 3), 'd': chip_id(z, y + 1, x + 3)}
    greet(list(ups.values()) + list(downs.values()))
    sems = (rs_send, rs_recv)
    started = []

    def ring_sum(base, ring, me, block, half, opp, fin):
        right, left = ups[ring], downs[ring]
        o, r, l = (me + 2) % SIDE, (me + 1) % SIDE, (me + 3) % SIDE
        one = push(half(block(o), 0), opp.at[0], sems, base, right)
        two = push(half(block(o), 1), opp.at[1], sems, base + 1, left)
        three = push(half(block(r), 1), half(fin.at[0], 1), sems, base + 2, right)
        four = push(half(block(l), 0), half(fin.at[1], 0), sems, base + 3, left)

        def forward():
            one.wait_recv()
            opp[0] = opp[0] + half(block(r), 0)[...]
            five = push(opp.at[0], half(fin.at[0], 0), sems, base + 4, right)
            two.wait_recv()
            opp[1] = opp[1] + half(block(l), 1)[...]
            six = push(opp.at[1], half(fin.at[1], 1), sems, base + 5, left)
            started.extend((one, two, three, four, five, six))

            def finish():
                for copy in (three, four, five, six):
                    copy.wait_recv()
                return block(me)[...] + fin[0] + fin[1]
            return finish
        return forward

    two_blocks = lambda ref, h: ref.at[pl.ds(2 * h, 2)]
    rows_half = lambda ref, h: ref.at[pl.ds(h * (n_rows // 2), n_rows // 2)]
    fwd_a = ring_sum(0, 'z', z, lambda i: part_a.at[i], two_blocks, opp1.at[0], fin1.at[0])
    fwd_b = ring_sum(6, 'd', x, lambda i: part_b.at[:, i], two_blocks, opp1.at[1], fin1.at[1])
    end_a, end_b = fwd_a(), fwd_b()
    sum1[0] = end_a()
    fwd_a = ring_sum(12, 'd', x, lambda i: sum1.at[0, i], rows_half, opp2.at[0], fin2.at[0])
    sum1[1] = end_b()
    fwd_b = ring_sum(18, 'z', z, lambda i: sum1.at[1, i], rows_half, opp2.at[1], fin2.at[1])
    end_a, end_b = fwd_a(), fwd_b()
    mine = jnp.concatenate([end_a(), end_b()], axis=1) * top_ref[...]
    mine = mine.astype(out_ref.dtype)
    for k in range(3):
        gath[k, z, y, x] = mine[:, k * third:(k + 1) * third]

    sems_ag = (ag_send, ag_recv)
    where = {'z': z, 'y': y, 'x': x}
    orders = ('xyz', 'yzx', 'zxy')

    def region(k, done, dim, i, h):
        index = []
        for name in 'zyx':
            if name == dim:
                index.append(i % SIDE)
            elif name in done:
                index.append(slice(None))
            else:
                index.append(where[name])
        return gath.at[(k, *index, pl.ds(h * (n_rows // 2), n_rows // 2))]

    for phase in range(3):
        firsts, seconds, thirds = [], [], []
        for k, order in enumerate(orders):
            dim, done = order[phase], order[:phase]
            spot = functools.partial(region, k, done, dim)
            me, base = where[dim], 18 * phase + 6 * k
            firsts.append((push(spot(me, 0), spot(me, 0), sems_ag, base, ups[dim]),
                           push(spot(me, 1), spot(me, 1), sems_ag, base + 1, downs[dim])))
        for k, order in enumerate(orders):
            dim, done = order[phase], order[:phase]
            spot = functools.partial(region, k, done, dim)
            me, base = where[dim], 18 * phase + 6 * k
            seconds.append((push(spot(me, 1), spot(me, 1), sems_ag, base + 2, ups[dim]),
                            push(spot(me, 0), spot(me, 0), sems_ag, base + 3, downs[dim])))
        for k, order in enumerate(orders):
            dim, done = order[phase], order[:phase]
            spot = functools.partial(region, k, done, dim)
            me, base = where[dim], 18 * phase + 6 * k
            firsts[k][0].wait_recv()
            one = push(spot(me + 3, 0), spot(me + 3, 0), sems_ag, base + 4, ups[dim])
            firsts[k][1].wait_recv()
            two = push(spot(me + 1, 1), spot(me + 1, 1), sems_ag, base + 5, downs[dim])
            thirds.append((one, two))
        for pair in seconds + thirds:
            for copy in pair:
                copy.wait_recv()
        for pair in firsts + seconds + thirds:
            started.extend(pair)
    lasts = []
    for k in range(3):
        last = pltpu.make_async_copy(gath.at[k], out_ref.at[:, :, :, :, pl.ds(k * third, third)], out_sem.at[k])
        last.start()
        lasts.append(last)
    for copy in started:
        copy.wait_send()
    for last in lasts:
        last.wait()


def combine(part_a, part_b, top):
    n_rows, width = part_a.shape[2:]
    blocks = (SIDE, SIDE, SIDE, n_rows)
    f32 = jnp.float32
    return pl.pallas_call(
        combine_kernel,
        out_shape=jax.ShapeDtypeStruct((*blocks, 2 * width), jnp.bfloat16),
        in_specs=[pl.BlockSpec(memory_space=pltpu.VMEM)] * 3,
        out_specs=pl.BlockSpec(memory_space=pl.ANY),
        scratch_shapes=[
            pltpu.VMEM((2, 2, 2, n_rows, width), f32),
            pltpu.VMEM((2, 2, SIDE, n_rows, width), f32),
            pltpu.VMEM((2, SIDE, n_rows, width), f32),
            pltpu.VMEM((2, 2, n_rows // 2, width), f32),
            pltpu.VMEM((2, 2, n_rows, width), f32),
            pltpu.VMEM((3, *blocks, 2 * width // 3), jnp.bfloat16),
            pltpu.SemaphoreType.DMA((24,)), pltpu.SemaphoreType.DMA((24,)),
            pltpu.SemaphoreType.DMA((54,)), pltpu.SemaphoreType.DMA((54,)),
            pltpu.SemaphoreType.DMA((3,)),
        ],
        compiler_params=pltpu.CompilerParams(collective_id=1, has_side_effects=True, vmem_limit_bytes=50 * 2 ** 20),
        name='combine',
    )(part_a, part_b, top)


def solution(mesh):
    row_spec = P(('dp', 'ep'), None)
    col_spec = P('ep', None, 'etp')
    in_specs = (row_spec, row_spec, row_spec, row_spec, col_spec, col_spec, P('ep', 'etp', None))

    def device_step(hidden, expert_ids, gate_wts, slot_pos, w_gate, w_up, w_down):
        rows, d_model = hidden.shape
        top_k = expert_ids.shape[1]
        local_experts, _, width = w_gate.shape
        z, y, x = coords()
        group = (x + y) % SIDE
        block = rows // SIDE ** 3

        def mine(a):
            a = a.reshape(SIDE, SIDE, SIDE, block, a.shape[1])
            picks = [lax.dynamic_index_in_dim(a[:, :, i], (group + SIDE - i) % SIDE, 1, keepdims=False) for i in range(SIDE)]
            return jnp.stack(picks, axis=1).reshape(SIDE * SIDE * block, a.shape[4])

        local = [w.transpose(0, 2, 1) for w in (w_gate, w_up)] + [w_down]
        local = jnp.stack([w.reshape(local_experts * width, d_model) for w in local])
        full = gather_weights(local)
        cols = 2 * SIDE * local_experts * width
        wg, wu, wd = full.reshape(3, cols, d_model)
        dim, place, core, expert, _ = jnp.unravel_index(jnp.arange(cols), (2, SIDE, 2, local_experts // 2, width))
        col_expert = (core * local_experts + dim * (local_experts // 2) + expert).astype(jnp.int32)

        hid, ids, gates, pos = mine(hidden), mine(expert_ids), mine(gate_wts), mine(slot_pos)
        kept = pos >= 0
        top = jnp.max(jnp.where(kept, gates, 0.0), axis=1, keepdims=True)
        top = jnp.where(top > 0, top, 1.0)
        rel = gates / top
        gate = jnp.zeros((hid.shape[0], cols), jnp.float32)
        for j in range(top_k):
            hit = (ids[:, j:j + 1] == col_expert[None, :]) & kept[:, j:j + 1]
            gate = jnp.where(hit, rel[:, j:j + 1], gate)
        nt = (((1,), (1,)), ((), ()))
        h_gate = lax.dot_general(hid, wg, nt, preferred_element_type=jnp.float32)
        h_up = lax.dot_general(hid, wu, nt, preferred_element_type=jnp.float32)
        act = lax.reduce_precision(jax.nn.silu(h_gate) * h_up, 8, 7)
        scaled = jnp.where(gate > 0, act * gate, 0.0)
        parts = jnp.concatenate(split3(scaled), axis=1)
        wd3 = jnp.concatenate([wd] * 3, axis=0)
        half = d_model // 2
        shape = (SIDE, SIDE, block, half)
        part_a = jnp.dot(parts, wd3[:, :half], preferred_element_type=jnp.float32).reshape(shape)
        part_b = jnp.dot(parts, wd3[:, half:], preferred_element_type=jnp.float32).reshape(shape)
        own_top = lax.dynamic_index_in_dim(top.reshape(SIDE * SIDE, block, 1), z * SIDE + x, 0, keepdims=False)
        return combine(part_a, part_b, own_top).reshape(rows, d_model)

    return jax.shard_map(device_step, mesh=mesh, in_specs=in_specs, out_specs=row_spec, check_vma=False)
```

```python
import functools

import jax
import jax.numpy as jnp
from jax import lax
from jax.experimental import pallas as pl
from jax.experimental.pallas import tpu as pltpu
from jax.sharding import PartitionSpec as P

MESH = pl.DeviceIdType.MESH
SIDE = 4


def split3(a):
    hi = lax.reduce_precision(a, 8, 7)
    rest = a - hi
    mid = lax.reduce_precision(rest, 8, 7)
    low = rest - mid
    return [v.astype(jnp.bfloat16) for v in (hi, mid, low)]


def split3_kernel(a):
    hi = a.astype(jnp.bfloat16)
    rest = a - hi.astype(jnp.float32)
    mid = rest.astype(jnp.bfloat16)
    low = (rest - mid.astype(jnp.float32)).astype(jnp.bfloat16)
    return hi, mid, low


def coords():
    chip = lax.axis_index('etp')
    return chip // (SIDE * SIDE), (chip // SIDE) % SIDE, chip % SIDE


def chip_id(z, y, x):
    return {'etp': ((z % SIDE) * SIDE + y % SIDE) * SIDE + x % SIDE}


def greet(partners):
    barrier = pltpu.get_barrier_semaphore()
    for device_id in partners:
        pl.semaphore_signal(barrier, inc=1, device_id=device_id, device_id_type=MESH)
    pl.semaphore_wait(barrier, len(partners))


def plan(src, dst, sems, n, device_id):
    send_sem, recv_sem = sems
    return pltpu.make_async_remote_copy(src_ref=src, dst_ref=dst, send_sem=send_sem.at[n], recv_sem=recv_sem.at[n],
                                        device_id=device_id, device_id_type=MESH)


def push(src, dst, sems, n, device_id):
    copy = plan(src, dst, sems, n, device_id)
    copy.start()
    return copy


def moe_kernel(hid_hbm, gate_hbm, spread_ref, w_ref, top_ref, out_ref,
               hid, gates, wbuf, part, opp1, fin1, sum1, opp2, fin2, own,
               in_sem, own_sem, ring_send, ring_recv, core_send, core_recv, rs_send, rs_recv, ag_send, ag_recv):
    z, y, x = coords()
    core = lax.axis_index('ep')
    other = {'ep': 1 - core}
    group = (x + y) % SIDE
    n_rows, depth = hid.shape[1:]
    width = part.shape[4]
    rows = w_ref.shape[1] // 2
    cols = 4 * rows
    f32 = jnp.float32
    ups = {'z': chip_id(z + 1, y, x), 'y': chip_id(z, y + 1, x), 'x': chip_id(z, y, x + 1), 'd': chip_id(z, y + 3, x + 1)}
    downs = {'z': chip_id(z + 3, y, x), 'y': chip_id(z, y + 3, x), 'x': chip_id(z, y, x + 3), 'd': chip_id(z, y + 1, x + 3)}

    loads = []
    for zi in range(SIDE):
        for xi in range(SIDE):
            n = zi * SIDE + xi
            chip = zi * SIDE * SIDE + ((group + SIDE - xi) % SIDE) * SIDE + xi
            loads.append(pltpu.make_async_copy(hid_hbm.at[chip], hid.at[n], in_sem.at[n]))
            loads.append(pltpu.make_async_copy(gate_hbm.at[chip], gates.at[n], in_sem.at[16 + n]))
    for load in loads:
        load.start()
    greet(list(ups.values()) + list(downs.values()) + [other])

    rings, cores = (ring_send, ring_recv), (core_send, core_recv)
    cut = (rows * 3 // 5, rows * 2 // 5)

    def span(d, h):
        return pl.ds(0, cut[d]) if h == 0 else pl.ds(cut[d], rows - cut[d])

    def src(d, h):
        start = d * rows + (cut[d] if h else 0)
        return w_ref.at[:, pl.ds(start, rows - cut[d] if h else cut[d]), :]

    def box(q, d, h):
        return wbuf.at[q, :, d, core, span(d, h), :]

    dims = 'xy'
    flights, firsts, seconds, thirds = [], [], [], []
    for d in range(2):
        firsts.append((push(src(d, 0), box(1, d, 0), rings, 6 * d, ups[dims[d]]),
                       push(src(d, 1), box(1, d, 1), rings, 6 * d + 1, downs[dims[d]])))
    owns = []
    for d in range(2):
        owns.append(push(w_ref.at[:, pl.ds(d * rows, rows), :], wbuf.at[0, :, d, core], cores, 7 * d, other))
    for d in range(2):
        seconds.append((push(src(d, 1), box(2, d, 1), rings, 6 * d + 2, ups[dims[d]]),
                        push(src(d, 0), box(2, d, 0), rings, 6 * d + 3, downs[dims[d]])))
    for d in range(2):
        wbuf[0, :, d, core] = w_ref[:, d * rows:(d + 1) * rows, :]
    for load in loads:
        load.wait()
    for copy in owns:
        copy.wait_recv()

    n_half = SIDE * SIDE // 2

    def compute(q, i):
        rows_in = n_half * n_rows
        tokens = hid[pl.ds(n_half * i, n_half)].reshape(rows_in, depth)
        gate = jnp.dot(gates[pl.ds(n_half * i, n_half)].reshape(rows_in, gates.shape[2]), spread_ref[...],
                       preferred_element_type=f32)
        both = lax.dot_general(tokens, wbuf[q, 0:2].reshape(2 * cols, depth), (((1,), (1,)), ((), ())),
                               preferred_element_type=f32)
        h_gate, h_up = both[:, :cols], both[:, cols:]
        act = (jax.nn.silu(h_gate) * h_up).astype(jnp.bfloat16).astype(f32)
        scaled = jnp.where(gate > 0, act * gate, 0.0)
        stack = jnp.concatenate(split3_kernel(scaled), axis=0)
        piece = width // 2
        for n in range(4):
            down = wbuf[q, 2, :, :, :, n * piece:(n + 1) * piece].reshape(cols, piece)
            out = jnp.dot(stack, down, preferred_element_type=f32)
            out = (out[:rows_in] + out[rows_in:2 * rows_in] + out[2 * rows_in:]).reshape(SIDE // 2, SIDE, n_rows, piece)
            where = (n // 2, pl.ds(SIDE // 2 * i, SIDE // 2), slice(None), slice(None), pl.ds((n % 2) * piece, piece))
            part[where] += out

    forwards = [plan(box(1, d, h), box(3, d, h), rings, 6 * d + 4 + h, (ups, downs)[h][dims[d]])
                for d in range(2) for h in range(2)]
    shares = [[plan(box(q, d, h), box(q, d, h), cores, 7 * d + 2 * q - 1 + h, other) for d in range(2) for h in range(2)]
              for q in range(1, SIDE)]
    arrivals = [[copy for pair in firsts for copy in pair], [copy for pair in seconds for copy in pair[::-1]], forwards]

    part[...] = jnp.zeros_like(part)

    @pl.loop(0, 2 * SIDE)
    def _(step):
        for q in range(1, SIDE):
            @pl.when(step == 2 * q - 1)
            def _():
                for n, copy in enumerate(arrivals[q - 1]):
                    copy.wait_recv()
                    if q == 1:
                        forwards[n].start()
                    shares[q - 1][n].start()

            @pl.when(step == 2 * q)
            def _():
                for copy in shares[q - 1]:
                    copy.wait_recv()
        compute(step // 2, step % 2)

    started = arrivals[0] + arrivals[1] + forwards + owns + [copy for share in shares for copy in share]

    sems = (rs_send, rs_recv)
    part_a, part_b = part.at[0], part.at[1]
    def ring_sum(base, ring, me, block, half, opp, fin):
        right, left = ups[ring], downs[ring]
        o, r, l = (me + 2) % SIDE, (me + 1) % SIDE, (me + 3) % SIDE
        one = push(half(block(o), 0), opp.at[0], sems, base, right)
        two = push(half(block(o), 1), opp.at[1], sems, base + 1, left)
        three = push(half(block(r), 1), half(fin.at[0], 1), sems, base + 2, right)
        four = push(half(block(l), 0), half(fin.at[1], 0), sems, base + 3, left)

        def forward():
            one.wait_recv()
            opp[0] = opp[0] + half(block(r), 0)[...]
            five = push(opp.at[0], half(fin.at[0], 0), sems, base + 4, right)
            two.wait_recv()
            opp[1] = opp[1] + half(block(l), 1)[...]
            six = push(opp.at[1], half(fin.at[1], 1), sems, base + 5, left)
            started.extend((one, two, three, four, five, six))

            def finish():
                for copy in (three, four, five, six):
                    copy.wait_recv()
                return block(me)[...] + fin[0] + fin[1]
            return finish
        return forward

    two_blocks = lambda ref, h: ref.at[pl.ds(2 * h, 2)]
    rows_half = lambda ref, h: ref.at[pl.ds(h * (n_rows // 2), n_rows // 2)]
    fwd_a = ring_sum(0, 'z', z, lambda i: part_a.at[i], two_blocks, opp1.at[0], fin1.at[0])
    fwd_b = ring_sum(6, 'd', x, lambda i: part_b.at[:, i], two_blocks, opp1.at[1], fin1.at[1])
    end_a, end_b = fwd_a(), fwd_b()
    sum1[0] = end_a()
    fwd_a = ring_sum(12, 'd', x, lambda i: sum1.at[0, i], rows_half, opp2.at[0], fin2.at[0])
    sum1[1] = end_b()
    fwd_b = ring_sum(18, 'z', z, lambda i: sum1.at[1, i], rows_half, opp2.at[1], fin2.at[1])
    end_a, end_b = fwd_a(), fwd_b()
    mine = jnp.concatenate([end_a(), end_b()], axis=1) * top_ref[...]
    mine = mine.astype(out_ref.dtype)
    own[...] = mine
    keep = pltpu.make_async_copy(own, out_ref.at[z, y, x], own_sem)
    keep.start()

    third = out_ref.shape[4] // 3
    sems_ag = (ag_send, ag_recv)
    where = {'z': z, 'y': y, 'x': x}
    orders = ('xyz', 'yzx', 'zxy')

    def owned(k, h):
        return own.at[pl.ds(h * (n_rows // 2), n_rows // 2), pl.ds(k * third, third)]

    def region(k, done, dim, i, h):
        index = []
        for name in 'zyx':
            if name == dim:
                index.append(i % SIDE)
            elif name in done:
                index.append(slice(None))
            else:
                index.append(where[name])
        return out_ref.at[(*index, pl.ds(h * (n_rows // 2), n_rows // 2), pl.ds(k * third, third))]

    for phase in range(3):
        if phase == 1:
            keep.wait()
        firsts, seconds, thirds = [], [], []
        for k, order in enumerate(orders):
            dim, done = order[phase], order[:phase]
            spot = functools.partial(region, k, done, dim)
            first = functools.partial(owned, k) if phase == 0 else functools.partial(spot, where[dim])
            me, base = where[dim], 18 * phase + 6 * k
            firsts.append((push(first(0), spot(me, 0), sems_ag, base, ups[dim]),
                           push(first(1), spot(me, 1), sems_ag, base + 1, downs[dim])))
        for k, order in enumerate(orders):
            dim, done = order[phase], order[:phase]
            spot = functools.partial(region, k, done, dim)
            first = functools.partial(owned, k) if phase == 0 else functools.partial(spot, where[dim])
            me, base = where[dim], 18 * phase + 6 * k
            seconds.append((push(first(1), spot(me, 1), sems_ag, base + 2, ups[dim]),
                            push(first(0), spot(me, 0), sems_ag, base + 3, downs[dim])))
        for k, order in enumerate(orders):
            dim, done = order[phase], order[:phase]
            spot = functools.partial(region, k, done, dim)
            me, base = where[dim], 18 * phase + 6 * k
            firsts[k][0].wait_recv()
            one = push(spot(me + 3, 0), spot(me + 3, 0), sems_ag, base + 4, ups[dim])
            firsts[k][1].wait_recv()
            two = push(spot(me + 1, 1), spot(me + 1, 1), sems_ag, base + 5, downs[dim])
            thirds.append((one, two))
        for pair in seconds + thirds:
            for copy in pair:
                copy.wait_recv()
        for pair in firsts + seconds + thirds:
            started.extend(pair)
    for copy in started:
        copy.wait_send()


def moe(hid, gates, spread, weights, top):
    blocks, n_rows, depth = hid.shape
    width = depth // 2
    rows = weights.shape[1] // 2
    f32, bf16 = jnp.float32, jnp.bfloat16
    dma = pltpu.SemaphoreType.DMA
    return pl.pallas_call(
        moe_kernel,
        out_shape=jax.ShapeDtypeStruct((SIDE, SIDE, SIDE, n_rows, depth), bf16),
        in_specs=[pl.BlockSpec(memory_space=pl.ANY)] * 2 + [pl.BlockSpec(memory_space=pltpu.VMEM)] * 3,
        out_specs=pl.BlockSpec(memory_space=pl.ANY),
        scratch_shapes=[
            pltpu.VMEM((SIDE * SIDE, n_rows, depth), bf16),
            pltpu.VMEM((SIDE * SIDE, n_rows, gates.shape[2]), bf16),
            pltpu.VMEM((SIDE, 3, 2, 2, rows, depth), bf16),
            pltpu.VMEM((2, SIDE, SIDE, n_rows, width), f32),
            pltpu.VMEM((2, 2, 2, n_rows, width), f32),
            pltpu.VMEM((2, 2, SIDE, n_rows, width), f32),
            pltpu.VMEM((2, SIDE, n_rows, width), f32),
            pltpu.VMEM((2, 2, n_rows // 2, width), f32),
            pltpu.VMEM((2, 2, n_rows, width), f32),
            pltpu.VMEM((n_rows, depth), bf16),
            dma((32,)), dma, dma((12,)), dma((12,)), dma((14,)), dma((14,)), dma((24,)), dma((24,)), dma((54,)), dma((54,)),
        ],
        compiler_params=pltpu.CompilerParams(collective_id=0, has_side_effects=True, vmem_limit_bytes=38 * 2 ** 20),
        name='moe',
    )(hid, gates, spread, weights, top)


def solution(mesh):
    row_spec = P(('dp', 'ep'), None)
    col_spec = P('ep', None, 'etp')
    in_specs = (row_spec, row_spec, row_spec, row_spec, col_spec, col_spec, P('ep', 'etp', None))

    def device_step(hidden, expert_ids, gate_wts, slot_pos, w_gate, w_up, w_down):
        rows, d_model = hidden.shape
        top_k = expert_ids.shape[1]
        local_experts, _, width = w_gate.shape
        experts = 2 * local_experts
        chips = SIDE ** 3
        block = rows // chips

        local = [w.transpose(0, 2, 1) for w in (w_gate, w_up)] + [w_down]
        local = jnp.stack([w.reshape(local_experts * width, d_model) for w in local])

        kept = slot_pos >= 0
        top = jnp.max(jnp.where(kept, gate_wts, 0.0), axis=1, keepdims=True)
        top = jnp.where(top > 0, top, 1.0)
        rel = gate_wts / top
        gate = jnp.zeros((rows, experts), jnp.float32)
        for j in range(top_k):
            hit = (expert_ids[:, j:j + 1] == jnp.arange(experts, dtype=jnp.int32)[None, :]) & kept[:, j:j + 1]
            gate = jnp.where(hit, rel[:, j:j + 1], gate)
        lanes = -(-3 * experts // 128) * 128
        gates = jnp.concatenate(split3(gate) + [jnp.zeros((rows, lanes - 3 * experts), jnp.bfloat16)], axis=1)

        cols = experts * width
        dim, core, expert, _ = jnp.unravel_index(jnp.arange(cols), (2, 2, local_experts // 2, width))
        col_expert = core * local_experts + dim * (local_experts // 2) + expert
        lane = jnp.arange(lanes)[:, None]
        spread = ((lane % experts == col_expert[None, :]) & (lane < 3 * experts)).astype(jnp.bfloat16)
        own_top = lax.dynamic_slice_in_dim(top, lax.axis_index('etp') * block, block, 0)
        out = moe(hidden.reshape(chips, block, d_model), gates.reshape(chips, block, lanes), spread, local, own_top)
        return out.reshape(rows, d_model)

    return jax.shard_map(device_step, mesh=mesh, in_specs=in_specs, out_specs=row_spec, check_vma=False)
```

```python
import functools

import jax
import jax.numpy as jnp
import numpy as np
from jax import lax
from jax.experimental import pallas as pl
from jax.experimental.pallas import tpu as pltpu
from jax.sharding import PartitionSpec as P

MESH = pl.DeviceIdType.MESH
SIDE = 4


def split3(a):
    hi = a.astype(jnp.bfloat16)
    rest = a - hi.astype(jnp.float32)
    mid = rest.astype(jnp.bfloat16)
    low = (rest - mid.astype(jnp.float32)).astype(jnp.bfloat16)
    return hi, mid, low


def coords():
    chip = lax.axis_index('etp')
    return chip // (SIDE * SIDE), (chip // SIDE) % SIDE, chip % SIDE


def chip_id(z, y, x):
    return {'etp': ((z % SIDE) * SIDE + y % SIDE) * SIDE + x % SIDE}


def greet(partners):
    barrier = pltpu.get_barrier_semaphore()
    for device_id in partners:
        pl.semaphore_signal(barrier, inc=1, device_id=device_id, device_id_type=MESH)
    pl.semaphore_wait(barrier, len(partners))


def plan(src, dst, sems, n, device_id):
    send_sem, recv_sem = sems
    return pltpu.make_async_remote_copy(src_ref=src, dst_ref=dst, send_sem=send_sem.at[n], recv_sem=recv_sem.at[n],
                                        device_id=device_id, device_id_type=MESH)


def push(src, dst, sems, n, device_id):
    copy = plan(src, dst, sems, n, device_id)
    copy.start()
    return copy


def moe_kernel(hid_hbm, ids_ref, gate_ref, pos_ref, spread_ref, w_ref, out_ref,
               hid, terms, gates, wbuf, part, opp1, fin1, sum1, opp2, fin2, own,
               in_sem, own_sem, ring_send, ring_recv, core_send, core_recv, rs_send, rs_recv, ag_send, ag_recv):
    z, y, x = coords()
    core = lax.axis_index('ep')
    other = {'ep': 1 - core}
    group = (x + y) % SIDE
    n_rows, depth = hid.shape[1:]
    width = part.shape[4]
    rows = w_ref.shape[1] // 2
    cols = 4 * rows
    f32 = jnp.float32
    ups = {'z': chip_id(z + 1, y, x), 'y': chip_id(z, y + 1, x), 'x': chip_id(z, y, x + 1), 'd': chip_id(z, y + 3, x + 1)}
    downs = {'z': chip_id(z + 3, y, x), 'y': chip_id(z, y + 3, x), 'x': chip_id(z, y, x + 3), 'd': chip_id(z, y + 1, x + 3)}

    loads = []
    for zi in range(SIDE):
        for xi in range(SIDE):
            n = zi * SIDE + xi
            chip = zi * SIDE * SIDE + ((group + SIDE - xi) % SIDE) * SIDE + xi
            loads.append(pltpu.make_async_copy(hid_hbm.at[chip], hid.at[n], in_sem.at[n]))
    for load in loads:
        load.start()
    greet(list(ups.values()) + list(downs.values()) + [other])

    rings, cores = (ring_send, ring_recv), (core_send, core_recv)
    cut = (rows * 3 // 5, rows * 2 // 5)

    def span(d, h):
        return pl.ds(0, cut[d]) if h == 0 else pl.ds(cut[d], rows - cut[d])

    def src(d, h):
        start = d * rows + (cut[d] if h else 0)
        return w_ref.at[:, pl.ds(start, rows - cut[d] if h else cut[d]), :]

    def box(q, d, h):
        return wbuf.at[q, :, d, core, span(d, h), :]

    dims = 'xy'
    flights, firsts, seconds, thirds = [], [], [], []
    for d in range(2):
        firsts.append((push(src(d, 0), box(1, d, 0), rings, 6 * d, ups[dims[d]]),
                       push(src(d, 1), box(1, d, 1), rings, 6 * d + 1, downs[dims[d]])))
    owns = []
    for d in range(2):
        owns.append(push(w_ref.at[:, pl.ds(d * rows, rows), :], wbuf.at[0, :, d, core], cores, 7 * d, other))
    for d in range(2):
        seconds.append((push(src(d, 1), box(2, d, 1), rings, 6 * d + 2, ups[dims[d]]),
                        push(src(d, 0), box(2, d, 0), rings, 6 * d + 3, downs[dims[d]])))
    for d in range(2):
        wbuf[0, :, d, core] = w_ref[:, d * rows:(d + 1) * rows, :]
    part[...] = jnp.zeros_like(part)

    kept = pos_ref[...] >= 0
    top = jnp.max(jnp.where(kept, gate_ref[...], 0.0), axis=0, keepdims=True)
    top = jnp.where(top > 0, top, 1.0)
    rel = jnp.where(kept, gate_ref[...] / top, 0.0)
    ids = ids_ref[...]
    experts = cols // 8
    expert = lax.broadcasted_iota(jnp.int32, (experts, ids.shape[1]), 0)
    dense = jnp.zeros((experts, ids.shape[1]), f32)
    for j in range(ids.shape[0]):
        dense = jnp.where(ids[j:j + 1] == expert, rel[j:j + 1], dense)
    dense = jnp.concatenate([dense, jnp.broadcast_to(top, (8, ids.shape[1]))], axis=0)
    for n, term in enumerate(split3(dense)):
        terms[pl.ds(n * (experts + 8), experts + 8)] = term.astype(f32)
    for zi in range(SIDE):
        for xi in range(SIDE):
            tile = zi * 8 + ((group + SIDE - xi) % SIDE) * 2 + xi // 2
            pair = terms[:, pl.ds(pl.multiple_of(tile * 2 * n_rows, 2 * n_rows), 2 * n_rows)].astype(jnp.bfloat16)
            spread = lax.dot_general(pair, spread_ref[...], (((0,), (0,)), ((), ())), preferred_element_type=f32)
            gates[zi * SIDE + xi] = spread[(xi % 2) * n_rows:(xi % 2 + 1) * n_rows]

    for load in loads:
        load.wait()
    for copy in owns:
        copy.wait_recv()

    n_half = SIDE * SIDE // 2

    def compute(q, i):
        rows_in = n_half * n_rows
        tokens = hid[pl.ds(n_half * i, n_half)].reshape(rows_in, depth)
        gate = gates[pl.ds(n_half * i, n_half)].reshape(rows_in, gates.shape[2])[:, :cols]
        both = lax.dot_general(tokens, wbuf[q, 0:2].reshape(2 * cols, depth), (((1,), (1,)), ((), ())),
                               preferred_element_type=f32)
        h_gate, h_up = both[:, :cols], both[:, cols:]
        act = (jax.nn.silu(h_gate) * h_up).astype(jnp.bfloat16).astype(f32)
        scaled = jnp.where(gate > 0, act * gate, 0.0)
        stack = jnp.concatenate(split3(scaled), axis=0)
        piece = width // 2
        for n in range(4):
            down = wbuf[q, 2, :, :, :, n * piece:(n + 1) * piece].reshape(cols, piece)
            out = jnp.dot(stack, down, preferred_element_type=f32)
            out = (out[:rows_in] + out[rows_in:2 * rows_in] + out[2 * rows_in:]).reshape(SIDE // 2, SIDE, n_rows, piece)
            where = (n // 2, pl.ds(SIDE // 2 * i, SIDE // 2), slice(None), slice(None), pl.ds((n % 2) * piece, piece))
            part[where] += out

    forwards = [plan(box(1, d, h), box(3, d, h), rings, 6 * d + 4 + h, (ups, downs)[h][dims[d]])
                for d in range(2) for h in range(2)]
    shares = [[plan(box(q, d, h), box(q, d, h), cores, 7 * d + 2 * q - 1 + h, other) for d in range(2) for h in range(2)]
              for q in range(1, SIDE)]
    arrivals = [[copy for pair in firsts for copy in pair], [copy for pair in seconds for copy in pair[::-1]], forwards]

    @pl.loop(0, 2 * SIDE)
    def _(step):
        for q in range(1, SIDE):
            @pl.when(step == 2 * q - 1)
            def _():
                for n, copy in enumerate(arrivals[q - 1]):
                    copy.wait_recv()
                    if q == 1:
                        forwards[n].start()
                    shares[q - 1][n].start()

            @pl.when(step == 2 * q)
            def _():
                for copy in shares[q - 1]:
                    copy.wait_recv()
        compute(step // 2, step % 2)

    started = arrivals[0] + arrivals[1] + forwards + owns + [copy for share in shares for copy in share]

    sems = (rs_send, rs_recv)
    part_a, part_b = part.at[0], part.at[1]
    def ring_sum(base, ring, me, block, half, opp, fin):
        right, left = ups[ring], downs[ring]
        o, r, l = (me + 2) % SIDE, (me + 1) % SIDE, (me + 3) % SIDE
        one = push(half(block(o), 0), opp.at[0], sems, base, right)
        two = push(half(block(o), 1), opp.at[1], sems, base + 1, left)
        three = push(half(block(r), 1), half(fin.at[0], 1), sems, base + 2, right)
        four = push(half(block(l), 0), half(fin.at[1], 0), sems, base + 3, left)

        def forward():
            one.wait_recv()
            opp[0] = opp[0] + half(block(r), 0)[...]
            five = push(opp.at[0], half(fin.at[0], 0), sems, base + 4, right)
            two.wait_recv()
            opp[1] = opp[1] + half(block(l), 1)[...]
            six = push(opp.at[1], half(fin.at[1], 1), sems, base + 5, left)
            started.extend((one, two, three, four, five, six))

            def finish():
                for copy in (three, four, five, six):
                    copy.wait_recv()
                return block(me)[...] + fin[0] + fin[1]
            return finish
        return forward

    two_blocks = lambda ref, h: ref.at[pl.ds(2 * h, 2)]
    rows_half = lambda ref, h: ref.at[pl.ds(h * (n_rows // 2), n_rows // 2)]
    fwd_a = ring_sum(0, 'z', z, lambda i: part_a.at[i], two_blocks, opp1.at[0], fin1.at[0])
    fwd_b = ring_sum(6, 'd', x, lambda i: part_b.at[:, i], two_blocks, opp1.at[1], fin1.at[1])
    end_a, end_b = fwd_a(), fwd_b()
    sum1[0] = end_a()
    fwd_a = ring_sum(12, 'd', x, lambda i: sum1.at[0, i], rows_half, opp2.at[0], fin2.at[0])
    sum1[1] = end_b()
    fwd_b = ring_sum(18, 'z', z, lambda i: sum1.at[1, i], rows_half, opp2.at[1], fin2.at[1])
    end_a, end_b = fwd_a(), fwd_b()
    mine = jnp.concatenate([end_a(), end_b()], axis=1) * gates[z * SIDE + x, :, pl.ds(cols, 1)]
    mine = mine.astype(out_ref.dtype)
    own[...] = mine
    keep = pltpu.make_async_copy(own, out_ref.at[z, y, x], own_sem)
    keep.start()

    third = out_ref.shape[4] // 3
    sems_ag = (ag_send, ag_recv)
    where = {'z': z, 'y': y, 'x': x}
    orders = ('xyz', 'yzx', 'zxy')

    def owned(k, h):
        return own.at[pl.ds(h * (n_rows // 2), n_rows // 2), pl.ds(k * third, third)]

    def region(k, done, dim, i, h):
        index = []
        for name in 'zyx':
            if name == dim:
                index.append(i % SIDE)
            elif name in done:
                index.append(slice(None))
            else:
                index.append(where[name])
        return out_ref.at[(*index, pl.ds(h * (n_rows // 2), n_rows // 2), pl.ds(k * third, third))]

    for phase in range(3):
        if phase == 1:
            keep.wait()
        firsts, seconds, thirds = [], [], []
        for k, order in enumerate(orders):
            dim, done = order[phase], order[:phase]
            spot = functools.partial(region, k, done, dim)
            first = functools.partial(owned, k) if phase == 0 else functools.partial(spot, where[dim])
            me, base = where[dim], 18 * phase + 6 * k
            firsts.append((push(first(0), spot(me, 0), sems_ag, base, ups[dim]),
                           push(first(1), spot(me, 1), sems_ag, base + 1, downs[dim])))
        for k, order in enumerate(orders):
            dim, done = order[phase], order[:phase]
            spot = functools.partial(region, k, done, dim)
            first = functools.partial(owned, k) if phase == 0 else functools.partial(spot, where[dim])
            me, base = where[dim], 18 * phase + 6 * k
            seconds.append((push(first(1), spot(me, 1), sems_ag, base + 2, ups[dim]),
                            push(first(0), spot(me, 0), sems_ag, base + 3, downs[dim])))
        for k, order in enumerate(orders):
            dim, done = order[phase], order[:phase]
            spot = functools.partial(region, k, done, dim)
            me, base = where[dim], 18 * phase + 6 * k
            firsts[k][0].wait_recv()
            one = push(spot(me + 3, 0), spot(me + 3, 0), sems_ag, base + 4, ups[dim])
            firsts[k][1].wait_recv()
            two = push(spot(me + 1, 1), spot(me + 1, 1), sems_ag, base + 5, downs[dim])
            thirds.append((one, two))
        for pair in seconds + thirds:
            for copy in pair:
                copy.wait_recv()
        for pair in firsts + seconds + thirds:
            started.extend(pair)
    for copy in started:
        copy.wait_send()


def moe(hid, ids, gate_wts, pos, spread, weights):
    blocks, n_rows, depth = hid.shape
    width = depth // 2
    rows = weights.shape[1] // 2
    f32, bf16 = jnp.float32, jnp.bfloat16
    dma = pltpu.SemaphoreType.DMA
    return pl.pallas_call(
        moe_kernel,
        out_shape=jax.ShapeDtypeStruct((SIDE, SIDE, SIDE, n_rows, depth), bf16),
        in_specs=[pl.BlockSpec(memory_space=pl.ANY)] + [pl.BlockSpec(memory_space=pltpu.VMEM)] * 5,
        out_specs=pl.BlockSpec(memory_space=pl.ANY),
        scratch_shapes=[
            pltpu.VMEM((SIDE * SIDE, n_rows, depth), bf16),
            pltpu.VMEM((spread.shape[0], ids.shape[1]), f32),
            pltpu.VMEM((SIDE * SIDE, n_rows, spread.shape[1]), f32),
            pltpu.VMEM((SIDE, 3, 2, 2, rows, depth), bf16),
            pltpu.VMEM((2, SIDE, SIDE, n_rows, width), f32),
            pltpu.VMEM((2, 2, 2, n_rows, width), f32),
            pltpu.VMEM((2, 2, SIDE, n_rows, width), f32),
            pltpu.VMEM((2, SIDE, n_rows, width), f32),
            pltpu.VMEM((2, 2, n_rows // 2, width), f32),
            pltpu.VMEM((2, 2, n_rows, width), f32),
            pltpu.VMEM((n_rows, depth), bf16),
            dma((16,)), dma, dma((12,)), dma((12,)), dma((14,)), dma((14,)), dma((24,)), dma((24,)), dma((54,)), dma((54,)),
        ],
        compiler_params=pltpu.CompilerParams(collective_id=0, has_side_effects=True, vmem_limit_bytes=38 * 2 ** 20),
        name='moe',
    )(hid, ids, gate_wts, pos, spread, weights)


def solution(mesh):
    row_spec = P(('dp', 'ep'), None)
    col_spec = P('ep', None, 'etp')
    in_specs = (row_spec, row_spec, row_spec, row_spec, col_spec, col_spec, P('ep', 'etp', None))

    def device_step(hidden, expert_ids, gate_wts, slot_pos, w_gate, w_up, w_down):
        rows, d_model = hidden.shape
        local_experts, _, width = w_gate.shape
        experts = 2 * local_experts
        chips = SIDE ** 3
        block = rows // chips

        local = [w.transpose(0, 2, 1) for w in (w_gate, w_up)] + [w_down]
        local = jnp.stack([w.reshape(local_experts * width, d_model) for w in local])

        cols = experts * width
        per_term = experts + 8
        dim, core, expert, _ = np.unravel_index(np.arange(cols), (2, 2, local_experts // 2, width))
        spread = np.zeros((3 * per_term, -(-(cols + 1) // 128) * 128), np.float32)
        for n in range(3):
            spread[n * per_term + core * local_experts + dim * (local_experts // 2) + expert, np.arange(cols)] = 1
            spread[n * per_term + experts, cols] = 1
        out = moe(hidden.reshape(chips, block, d_model), expert_ids.T, gate_wts.T, slot_pos.T,
                  jnp.asarray(spread, jnp.bfloat16), local)
        return out.reshape(rows, d_model)

    return jax.shard_map(device_step, mesh=mesh, in_specs=in_specs, out_specs=row_spec, check_vma=False)
```

```python
import functools

import jax
import jax.numpy as jnp
import numpy as np
from jax import lax
from jax.experimental import pallas as pl
from jax.experimental.pallas import tpu as pltpu
from jax.sharding import PartitionSpec as P

MESH = pl.DeviceIdType.MESH
SIDE = 4


def split3(a):
    hi = a.astype(jnp.bfloat16)
    rest = a - hi.astype(jnp.float32)
    mid = rest.astype(jnp.bfloat16)
    low = (rest - mid.astype(jnp.float32)).astype(jnp.bfloat16)
    return hi, mid, low


def coords():
    chip = lax.axis_index('etp')
    return chip // (SIDE * SIDE), (chip // SIDE) % SIDE, chip % SIDE


def chip_id(z, y, x):
    return {'etp': ((z % SIDE) * SIDE + y % SIDE) * SIDE + x % SIDE}


def greet(partners):
    barrier = pltpu.get_barrier_semaphore()
    for device_id in partners:
        pl.semaphore_signal(barrier, inc=1, device_id=device_id, device_id_type=MESH)
    pl.semaphore_wait(barrier, len(partners))


def plan(src, dst, sems, n, device_id):
    send_sem, recv_sem = sems
    return pltpu.make_async_remote_copy(src_ref=src, dst_ref=dst, send_sem=send_sem.at[n], recv_sem=recv_sem.at[n],
                                        device_id=device_id, device_id_type=MESH)


def push(src, dst, sems, n, device_id):
    copy = plan(src, dst, sems, n, device_id)
    copy.start()
    return copy


def moe_kernel(hid_hbm, ids_ref, gate_ref, pos_ref, spread_ref, w_ref, out_ref,
               hid, terms, gates, wbuf, part, opp1, fin1, sum1, opp2, fin2, own,
               in_sem, own_sem, ring_send, ring_recv, core_send, core_recv, rs_send, rs_recv, ag_send, ag_recv):
    z, y, x = coords()
    core = lax.axis_index('ep')
    other = {'ep': 1 - core}
    group = (x + y) % SIDE
    n_rows, depth = hid.shape[1:]
    width = part.shape[4]
    rows = w_ref.shape[1] // 2
    cols = 4 * rows
    f32 = jnp.float32
    ups = {'z': chip_id(z + 1, y, x), 'y': chip_id(z, y + 1, x), 'x': chip_id(z, y, x + 1), 'd': chip_id(z, y + 3, x + 1)}
    downs = {'z': chip_id(z + 3, y, x), 'y': chip_id(z, y + 3, x), 'x': chip_id(z, y, x + 3), 'd': chip_id(z, y + 1, x + 3)}

    loads = []
    for zi in range(SIDE):
        for xi in range(SIDE):
            n = zi * SIDE + xi
            chip = zi * SIDE * SIDE + ((group + SIDE - xi) % SIDE) * SIDE + xi
            loads.append(pltpu.make_async_copy(hid_hbm.at[chip], hid.at[n], in_sem.at[n]))
    for load in loads:
        load.start()
    greet(list(ups.values()) + list(downs.values()) + [other])

    rings, cores = (ring_send, ring_recv), (core_send, core_recv)
    cut = (rows * 3 // 5, rows * 2 // 5)

    def span(d, h):
        return pl.ds(0, cut[d]) if h == 0 else pl.ds(cut[d], rows - cut[d])

    def src(d, h):
        start = d * rows + (cut[d] if h else 0)
        return w_ref.at[:, pl.ds(start, rows - cut[d] if h else cut[d]), :]

    def box(q, d, h):
        return wbuf.at[q, :, d, core, span(d, h), :]

    dims = 'xy'
    flights, firsts, seconds, thirds = [], [], [], []
    for d in range(2):
        firsts.append((push(src(d, 0), box(1, d, 0), rings, 6 * d, ups[dims[d]]),
                       push(src(d, 1), box(1, d, 1), rings, 6 * d + 1, downs[dims[d]])))
    owns = []
    for d in range(2):
        owns.append(push(w_ref.at[:, pl.ds(d * rows, rows), :], wbuf.at[0, :, d, core], cores, 7 * d, other))
    for d in range(2):
        seconds.append((push(src(d, 1), box(2, d, 1), rings, 6 * d + 2, ups[dims[d]]),
                        push(src(d, 0), box(2, d, 0), rings, 6 * d + 3, downs[dims[d]])))
    for d in range(2):
        wbuf[0, :, d, core] = w_ref[:, d * rows:(d + 1) * rows, :]
    part[...] = jnp.zeros_like(part)

    kept = pos_ref[...] >= 0
    top = jnp.max(jnp.where(kept, gate_ref[...], 0.0), axis=0, keepdims=True)
    top = jnp.where(top > 0, top, 1.0)
    rel = jnp.where(kept, gate_ref[...] / top, 0.0)
    ids = ids_ref[...]
    experts = cols // 8
    expert = lax.broadcasted_iota(jnp.int32, (experts, ids.shape[1]), 0)
    dense = jnp.zeros((experts, ids.shape[1]), f32)
    for j in range(ids.shape[0]):
        dense = jnp.where(ids[j:j + 1] == expert, rel[j:j + 1], dense)
    dense = jnp.concatenate([dense, jnp.broadcast_to(top, (8, ids.shape[1]))], axis=0)
    for n, term in enumerate(split3(dense)):
        terms[pl.ds(n * (experts + 8), experts + 8)] = term.astype(f32)
    for zi in range(SIDE):
        for xi in range(SIDE):
            tile = zi * 8 + ((group + SIDE - xi) % SIDE) * 2 + xi // 2
            pair = terms[:, pl.ds(pl.multiple_of(tile * 2 * n_rows, 2 * n_rows), 2 * n_rows)].astype(jnp.bfloat16)
            spread = lax.dot_general(pair, spread_ref[...], (((0,), (0,)), ((), ())), preferred_element_type=f32)
            gates[zi * SIDE + xi] = spread[(xi % 2) * n_rows:(xi % 2 + 1) * n_rows]

    for load in loads:
        load.wait()
    for copy in owns:
        copy.wait_recv()

    n_half = SIDE * SIDE // 2

    def compute(q, i):
        rows_in = n_half * n_rows
        tokens = hid[pl.ds(n_half * i, n_half)].reshape(rows_in, depth)
        gate = gates[pl.ds(n_half * i, n_half)].reshape(rows_in, gates.shape[2])[:, :cols]
        h_gate = lax.dot_general(tokens, wbuf[q, 0].reshape(cols, depth), (((1,), (1,)), ((), ())),
                                 preferred_element_type=f32)
        h_up = lax.dot_general(tokens, wbuf[q, 1].reshape(cols, depth), (((1,), (1,)), ((), ())),
                               preferred_element_type=f32)
        act = (jax.nn.silu(h_gate) * h_up).astype(jnp.bfloat16).astype(f32)
        scaled = jnp.where(gate > 0, act * gate, 0.0)
        stack = jnp.concatenate(split3(scaled), axis=1)
        for n in range(2):
            down = wbuf[q, 2, :, :, :, n * width:(n + 1) * width].reshape(cols, width)
            out = jnp.dot(stack, jnp.concatenate([down] * 3, axis=0), preferred_element_type=f32)
            part[n, pl.ds(SIDE // 2 * i, SIDE // 2)] += out.reshape(SIDE // 2, SIDE, n_rows, width)

    forwards = [plan(box(1, d, h), box(3, d, h), rings, 6 * d + 4 + h, (ups, downs)[h][dims[d]])
                for d in range(2) for h in range(2)]
    shares = [[plan(box(q, d, h), box(q, d, h), cores, 7 * d + 2 * q - 1 + h, other) for d in range(2) for h in range(2)]
              for q in range(1, SIDE)]
    arrivals = [[copy for pair in firsts for copy in pair], [copy for pair in seconds for copy in pair[::-1]], forwards]

    @pl.loop(0, 2 * SIDE)
    def _(step):
        for q in range(1, SIDE):
            @pl.when(step == 2 * q - 1)
            def _():
                for n, copy in enumerate(arrivals[q - 1]):
                    copy.wait_recv()
                    if q == 1:
                        forwards[n].start()
                    shares[q - 1][n].start()

            @pl.when(step == 2 * q)
            def _():
                for copy in shares[q - 1]:
                    copy.wait_recv()
        compute(step // 2, step % 2)

    started = arrivals[0] + arrivals[1] + forwards + owns + [copy for share in shares for copy in share]

    sems = (rs_send, rs_recv)
    part_a, part_b = part.at[0], part.at[1]
    def ring_sum(base, ring, me, block, half, opp, fin):
        right, left = ups[ring], downs[ring]
        o, r, l = (me + 2) % SIDE, (me + 1) % SIDE, (me + 3) % SIDE
        one = push(half(block(o), 0), opp.at[0], sems, base, right)
        two = push(half(block(o), 1), opp.at[1], sems, base + 1, left)
        three = push(half(block(r), 1), half(fin.at[0], 1), sems, base + 2, right)
        four = push(half(block(l), 0), half(fin.at[1], 0), sems, base + 3, left)

        def forward():
            one.wait_recv()
            opp[0] = opp[0] + half(block(r), 0)[...]
            five = push(opp.at[0], half(fin.at[0], 0), sems, base + 4, right)
            two.wait_recv()
            opp[1] = opp[1] + half(block(l), 1)[...]
            six = push(opp.at[1], half(fin.at[1], 1), sems, base + 5, left)
            started.extend((one, two, three, four, five, six))

            def finish():
                for copy in (three, four, five, six):
                    copy.wait_recv()
                return block(me)[...] + fin[0] + fin[1]
            return finish
        return forward

    two_blocks = lambda ref, h: ref.at[pl.ds(2 * h, 2)]
    rows_half = lambda ref, h: ref.at[pl.ds(h * (n_rows // 2), n_rows // 2)]
    fwd_a = ring_sum(0, 'z', z, lambda i: part_a.at[i], two_blocks, opp1.at[0], fin1.at[0])
    fwd_b = ring_sum(6, 'd', x, lambda i: part_b.at[:, i], two_blocks, opp1.at[1], fin1.at[1])
    end_a, end_b = fwd_a(), fwd_b()
    sum1[0] = end_a()
    fwd_a = ring_sum(12, 'd', x, lambda i: sum1.at[0, i], rows_half, opp2.at[0], fin2.at[0])
    sum1[1] = end_b()
    fwd_b = ring_sum(18, 'z', z, lambda i: sum1.at[1, i], rows_half, opp2.at[1], fin2.at[1])
    end_a, end_b = fwd_a(), fwd_b()
    mine = jnp.concatenate([end_a(), end_b()], axis=1) * gates[z * SIDE + x, :, pl.ds(cols, 1)]
    mine = mine.astype(out_ref.dtype)
    own[...] = mine
    keep = pltpu.make_async_copy(own, out_ref.at[z, y, x], own_sem)
    keep.start()

    third = out_ref.shape[4] // 3
    sems_ag = (ag_send, ag_recv)
    where = {'z': z, 'y': y, 'x': x}
    orders = ('xyz', 'yzx', 'zxy')

    def owned(k, h):
        return own.at[pl.ds(h * (n_rows // 2), n_rows // 2), pl.ds(k * third, third)]

    def region(k, done, dim, i, h):
        index = []
        for name in 'zyx':
            if name == dim:
                index.append(i % SIDE)
            elif name in done:
                index.append(slice(None))
            else:
                index.append(where[name])
        return out_ref.at[(*index, pl.ds(h * (n_rows // 2), n_rows // 2), pl.ds(k * third, third))]

    for phase in range(3):
        if phase == 1:
            keep.wait()
        firsts, seconds, thirds = [], [], []
        for k, order in enumerate(orders):
            dim, done = order[phase], order[:phase]
            spot = functools.partial(region, k, done, dim)
            first = functools.partial(owned, k) if phase == 0 else functools.partial(spot, where[dim])
            me, base = where[dim], 18 * phase + 6 * k
            firsts.append((push(first(0), spot(me, 0), sems_ag, base, ups[dim]),
                           push(first(1), spot(me, 1), sems_ag, base + 1, downs[dim])))
        for k, order in enumerate(orders):
            dim, done = order[phase], order[:phase]
            spot = functools.partial(region, k, done, dim)
            first = functools.partial(owned, k) if phase == 0 else functools.partial(spot, where[dim])
            me, base = where[dim], 18 * phase + 6 * k
            seconds.append((push(first(1), spot(me, 1), sems_ag, base + 2, ups[dim]),
                            push(first(0), spot(me, 0), sems_ag, base + 3, downs[dim])))
        for k, order in enumerate(orders):
            dim, done = order[phase], order[:phase]
            spot = functools.partial(region, k, done, dim)
            me, base = where[dim], 18 * phase + 6 * k
            firsts[k][0].wait_recv()
            one = push(spot(me + 3, 0), spot(me + 3, 0), sems_ag, base + 4, ups[dim])
            firsts[k][1].wait_recv()
            two = push(spot(me + 1, 1), spot(me + 1, 1), sems_ag, base + 5, downs[dim])
            thirds.append((one, two))
        for pair in seconds + thirds:
            for copy in pair:
                copy.wait_recv()
        for pair in firsts + seconds + thirds:
            started.extend(pair)
    for copy in started:
        copy.wait_send()


def moe(hid, ids, gate_wts, pos, spread, weights):
    blocks, n_rows, depth = hid.shape
    width = depth // 2
    rows = weights.shape[1] // 2
    f32, bf16 = jnp.float32, jnp.bfloat16
    dma = pltpu.SemaphoreType.DMA
    return pl.pallas_call(
        moe_kernel,
        out_shape=jax.ShapeDtypeStruct((SIDE, SIDE, SIDE, n_rows, depth), bf16),
        in_specs=[pl.BlockSpec(memory_space=pl.ANY)] + [pl.BlockSpec(memory_space=pltpu.VMEM)] * 5,
        out_specs=pl.BlockSpec(memory_space=pl.ANY),
        scratch_shapes=[
            pltpu.VMEM((SIDE * SIDE, n_rows, depth), bf16),
            pltpu.VMEM((spread.shape[0], ids.shape[1]), f32),
            pltpu.VMEM((SIDE * SIDE, n_rows, spread.shape[1]), f32),
            pltpu.VMEM((SIDE, 3, 2, 2, rows, depth), bf16),
            pltpu.VMEM((2, SIDE, SIDE, n_rows, width), f32),
            pltpu.VMEM((2, 2, 2, n_rows, width), f32),
            pltpu.VMEM((2, 2, SIDE, n_rows, width), f32),
            pltpu.VMEM((2, SIDE, n_rows, width), f32),
            pltpu.VMEM((2, 2, n_rows // 2, width), f32),
            pltpu.VMEM((2, 2, n_rows, width), f32),
            pltpu.VMEM((n_rows, depth), bf16),
            dma((16,)), dma, dma((12,)), dma((12,)), dma((14,)), dma((14,)), dma((24,)), dma((24,)), dma((54,)), dma((54,)),
        ],
        compiler_params=pltpu.CompilerParams(collective_id=0, has_side_effects=True, vmem_limit_bytes=38 * 2 ** 20),
        name='moe',
    )(hid, ids, gate_wts, pos, spread, weights)


def solution(mesh):
    row_spec = P(('dp', 'ep'), None)
    col_spec = P('ep', None, 'etp')
    in_specs = (row_spec, row_spec, row_spec, row_spec, col_spec, col_spec, P('ep', 'etp', None))

    def device_step(hidden, expert_ids, gate_wts, slot_pos, w_gate, w_up, w_down):
        rows, d_model = hidden.shape
        local_experts, _, width = w_gate.shape
        experts = 2 * local_experts
        chips = SIDE ** 3
        block = rows // chips

        local = [w.transpose(0, 2, 1) for w in (w_gate, w_up)] + [w_down]
        local = jnp.stack([w.reshape(local_experts * width, d_model) for w in local])

        cols = experts * width
        per_term = experts + 8
        dim, core, expert, _ = np.unravel_index(np.arange(cols), (2, 2, local_experts // 2, width))
        spread = np.zeros((3 * per_term, -(-(cols + 1) // 128) * 128), np.float32)
        for n in range(3):
            spread[n * per_term + core * local_experts + dim * (local_experts // 2) + expert, np.arange(cols)] = 1
            spread[n * per_term + experts, cols] = 1
        out = moe(hidden.reshape(chips, block, d_model), expert_ids.T, gate_wts.T, slot_pos.T,
                  jnp.asarray(spread, jnp.bfloat16), local)
        return out.reshape(rows, d_model)

    return jax.shard_map(device_step, mesh=mesh, in_specs=in_specs, out_specs=row_spec, check_vma=False)
```

```python
import functools

import jax
import jax.numpy as jnp
import numpy as np
from jax import lax
from jax.experimental import pallas as pl
from jax.experimental.pallas import tpu as pltpu
from jax.sharding import PartitionSpec as P

MESH = pl.DeviceIdType.MESH
SIDE = 4
PLACES = [(2, 2), (2, 1), (1, 2), (2, 3), (3, 2), (2, 0), (0, 2), (1, 1),
          (3, 1), (1, 3), (3, 3), (0, 1), (1, 0), (0, 3), (3, 0), (0, 0)]


def split3(a):
    hi = a.astype(jnp.bfloat16)
    rest = a - hi.astype(jnp.float32)
    mid = rest.astype(jnp.bfloat16)
    low = (rest - mid.astype(jnp.float32)).astype(jnp.bfloat16)
    return hi, mid, low


def coords():
    chip = lax.axis_index('etp')
    return chip // (SIDE * SIDE), (chip // SIDE) % SIDE, chip % SIDE


def chip_id(z, y, x):
    return {'etp': ((z % SIDE) * SIDE + y % SIDE) * SIDE + x % SIDE}


def greet(partners):
    barrier = pltpu.get_barrier_semaphore()
    for device_id in partners:
        pl.semaphore_signal(barrier, inc=1, device_id=device_id, device_id_type=MESH)
    pl.semaphore_wait(barrier, len(partners))


def plan(src, dst, sems, n, device_id):
    send_sem, recv_sem = sems
    return pltpu.make_async_remote_copy(src_ref=src, dst_ref=dst, send_sem=send_sem.at[n], recv_sem=recv_sem.at[n],
                                        device_id=device_id, device_id_type=MESH)


def push(src, dst, sems, n, device_id):
    copy = plan(src, dst, sems, n, device_id)
    copy.start()
    return copy


def moe_kernel(hid_hbm, ids_ref, gate_ref, pos_ref, spread_ref, w_ref, out_ref,
               hid, terms, gates, wbuf, part, opp1, fin1, sum1, opp2, fin2, own,
               in_sem, own_sem, ring_send, ring_recv, core_send, core_recv, rs_send, rs_recv, ag_send, ag_recv):
    z, y, x = coords()
    core = lax.axis_index('ep')
    other = {'ep': 1 - core}
    group = (x + y) % SIDE
    n_rows, depth = hid.shape[1:]
    width = part.shape[3]
    rows = w_ref.shape[1] // 2
    cols = 4 * rows
    f32 = jnp.float32
    ups = {'z': chip_id(z + 1, y, x), 'y': chip_id(z, y + 1, x), 'x': chip_id(z, y, x + 1), 'd': chip_id(z, y + 3, x + 1)}
    downs = {'z': chip_id(z + 3, y, x), 'y': chip_id(z, y + 3, x), 'x': chip_id(z, y, x + 3), 'd': chip_id(z, y + 1, x + 3)}

    loads = []
    spots = []
    for n, (dz, dx) in enumerate(PLACES):
        zi, xi = (z + dz) % SIDE, (x + dx) % SIDE
        chip = (zi * SIDE + (group + SIDE - xi) % SIDE) * SIDE + xi
        spots.append(chip)
        loads.append(pltpu.make_async_copy(hid_hbm.at[chip], hid.at[n], in_sem.at[n]))
    for load in loads:
        load.start()
    greet(list(ups.values()) + list(downs.values()) + [other])

    rings, cores = (ring_send, ring_recv), (core_send, core_recv)
    cut = (rows * 3 // 5, rows * 2 // 5)

    def span(d, h):
        return pl.ds(0, cut[d]) if h == 0 else pl.ds(cut[d], rows - cut[d])

    def src(d, h):
        start = d * rows + (cut[d] if h else 0)
        return w_ref.at[:, pl.ds(start, rows - cut[d] if h else cut[d]), :]

    def box(q, d, h):
        return wbuf.at[q, :, d, core, span(d, h), :]

    dims = 'xy'
    flights, firsts, seconds, thirds = [], [], [], []
    for d in range(2):
        firsts.append((push(src(d, 0), box(1, d, 0), rings, 6 * d, ups[dims[d]]),
                       push(src(d, 1), box(1, d, 1), rings, 6 * d + 1, downs[dims[d]])))
    owns = []
    for d in range(2):
        owns.append(push(w_ref.at[:, pl.ds(d * rows, rows), :], wbuf.at[0, :, d, core], cores, 7 * d, other))
    for d in range(2):
        seconds.append((push(src(d, 1), box(2, d, 1), rings, 6 * d + 2, ups[dims[d]]),
                        push(src(d, 0), box(2, d, 0), rings, 6 * d + 3, downs[dims[d]])))
    for d in range(2):
        wbuf[0, :, d, core] = w_ref[:, d * rows:(d + 1) * rows, :]
    part[...] = jnp.zeros_like(part)

    kept = pos_ref[...] >= 0
    top = jnp.max(jnp.where(kept, gate_ref[...], 0.0), axis=0, keepdims=True)
    top = jnp.where(top > 0, top, 1.0)
    rel = jnp.where(kept, gate_ref[...] / top, 0.0)
    ids = ids_ref[...]
    experts = cols // 8
    expert = lax.broadcasted_iota(jnp.int32, (experts, ids.shape[1]), 0)
    dense = jnp.zeros((experts, ids.shape[1]), f32)
    for j in range(ids.shape[0]):
        dense = jnp.where(ids[j:j + 1] == expert, rel[j:j + 1], dense)
    dense = jnp.concatenate([dense, jnp.broadcast_to(top, (8, ids.shape[1]))], axis=0)
    for n, term in enumerate(split3(dense)):
        terms[pl.ds(n * (experts + 8), experts + 8)] = term.astype(f32)
    for n, chip in enumerate(spots):
        start = pl.multiple_of((chip // 2) * 2 * n_rows, 2 * n_rows)
        pair = terms[:, pl.ds(start, 2 * n_rows)].astype(jnp.bfloat16)
        spread = lax.dot_general(pair, spread_ref[...], (((0,), (0,)), ((), ())), preferred_element_type=f32)
        gates[n] = jnp.where(chip % 2 == 1, spread[n_rows:], spread[:n_rows])

    for load in loads:
        load.wait()
    for copy in owns:
        copy.wait_recv()

    n_half = len(PLACES) // 2

    def compute(q, i):
        rows_in = n_half * n_rows
        tokens = hid[pl.ds(n_half * i, n_half)].reshape(rows_in, depth)
        gate = gates[pl.ds(n_half * i, n_half)].reshape(rows_in, gates.shape[2])[:, :cols]
        h_gate = lax.dot_general(tokens, wbuf[q, 0].reshape(cols, depth), (((1,), (1,)), ((), ())),
                                 preferred_element_type=f32)
        h_up = lax.dot_general(tokens, wbuf[q, 1].reshape(cols, depth), (((1,), (1,)), ((), ())),
                               preferred_element_type=f32)
        act = (jax.nn.silu(h_gate) * h_up).astype(jnp.bfloat16).astype(f32)
        scaled = jnp.where(gate > 0, act * gate, 0.0)
        stack = jnp.concatenate(split3(scaled), axis=1)
        for n in range(2):
            down = wbuf[q, 2, :, :, :, n * width:(n + 1) * width].reshape(cols, width)
            out = jnp.dot(stack, jnp.concatenate([down] * 3, axis=0), preferred_element_type=f32)
            part[n, pl.ds(n_half * i, n_half)] += out.reshape(n_half, n_rows, width)

    forwards = [plan(box(1, d, h), box(3, d, h), rings, 6 * d + 4 + h, (ups, downs)[h][dims[d]])
                for d in range(2) for h in range(2)]
    shares = [[plan(box(q, d, h), box(q, d, h), cores, 7 * d + 2 * q - 1 + h, other) for d in range(2) for h in range(2)]
              for q in range(1, SIDE)]
    arrivals = [[copy for pair in firsts for copy in pair], [copy for pair in seconds for copy in pair[::-1]], forwards]

    @pl.loop(0, 2 * SIDE - 1)
    def _(step):
        for q in range(1, SIDE):
            @pl.when(step == 2 * q - 1)
            def _():
                for n, copy in enumerate(arrivals[q - 1]):
                    copy.wait_recv()
                    if q == 1:
                        forwards[n].start()
                    shares[q - 1][n].start()

            @pl.when(step == 2 * q)
            def _():
                for copy in shares[q - 1]:
                    copy.wait_recv()
        compute(step // 2, step % 2)

    started = arrivals[0] + arrivals[1] + forwards + owns + [copy for share in shares for copy in share]

    sems = (rs_send, rs_recv)
    rings_of = ('zd', 'dz')
    offsets = (2, 1, 3, 0)

    def half(ref, h):
        return ref.at[pl.ds(h * (n_rows // 2), n_rows // 2)]

    def block(p, i, j):
        return part.at[p, PLACES.index((i, j) if p == 0 else (j, i))]

    ways = [(ups[r[0]], downs[r[0]]) for r in rings_of]
    first = [[[plan(half(block(p, 2, j), h), opp1.at[p, h, j], sems, 24 * p + 6 * j + h, ways[p][h])
               for h in range(2)] for j in range(SIDE)] for p in range(2)]
    direct = [[[plan(half(block(p, 3 if h else 1, j), 1 - h), half(fin1.at[p, h, j], 1 - h), sems, 24 * p + 6 * j + 2 + h, ways[p][h])
                for h in range(2)] for j in range(SIDE)] for p in range(2)]
    onward = [[[plan(opp1.at[p, h, j], half(fin1.at[p, h, j], h), sems, 24 * p + 6 * j + 4 + h, ways[p][h])
                for h in range(2)] for j in range(SIDE)] for p in range(2)]
    for group_of in (first, direct, onward):
        started += [copy for per_part in group_of for pair in per_part for copy in pair]

    def launch(table, k):
        if k < SIDE:
            for p in range(2):
                for copy in table[p][offsets[k]]:
                    copy.start()

    launch(first, 0)
    launch(direct, 0)
    launch(first, 1)
    compute(SIDE - 1, 1)

    ways2 = [(ups[r[1]], downs[r[1]]) for r in rings_of]
    first2, direct2 = [[None] * 2 for _ in range(2)], [[None] * 2 for _ in range(2)]

    def finish(k):
        j = offsets[k]
        for p in range(2):
            for h in range(2):
                direct[p][j][h].wait_recv()
                onward[p][j][h].wait_recv()
            sum1[p, j] = block(p, 0, j)[...] + fin1[p, 0, j] + fin1[p, 1, j]
            base = 48 + 6 * p
            if j == 2:
                for h in range(2):
                    first2[p][h] = push(half(sum1.at[p, j], h), opp2.at[p, h], sems, base + h, ways2[p][h])
            elif j:
                h = 0 if j == 1 else 1
                direct2[p][h] = push(half(sum1.at[p, j], 1 - h), half(fin2.at[p, h], 1 - h), sems, base + 2 + h, ways2[p][h])

    for k in range(SIDE):
        j = offsets[k]
        for p in range(2):
            for h in range(2):
                first[p][j][h].wait_recv()
                opp1[p, h, j] = opp1[p, h, j] + half(block(p, 3 if h else 1, j), h)[...]
                onward[p][j][h].start()
        launch(direct, k + 1)
        launch(first, k + 2)
        if k:
            finish(k - 1)
    finish(SIDE - 1)
    onward2 = [[None] * 2 for _ in range(2)]
    for p in range(2):
        for h in range(2):
            first2[p][h].wait_recv()
            opp2[p, h] = opp2[p, h] + half(sum1.at[p, 3 if h else 1], h)[...]
            onward2[p][h] = push(opp2.at[p, h], half(fin2.at[p, h], h), sems, 52 + 6 * p + h, ways2[p][h])
    total = []
    for p in range(2):
        for h in range(2):
            direct2[p][h].wait_recv()
            onward2[p][h].wait_recv()
        total.append(sum1[p, 0] + fin2[p, 0] + fin2[p, 1])
    for table in (first2, direct2, onward2):
        started += [copy for pair in table for copy in pair]
    mine = jnp.concatenate(total, axis=1) * gates[len(PLACES) - 1, :, pl.ds(cols, 1)]
    own[...] = mine.astype(out_ref.dtype)
    keep = pltpu.make_async_copy(own, out_ref.at[z, y, x], own_sem)
    keep.start()

    third = out_ref.shape[4] // 3
    sems_ag = (ag_send, ag_recv)
    where = {'z': z, 'y': y, 'x': x}
    orders = ('xyz', 'yzx', 'zxy')
    shifts = (0, 3, 1, 2)
    colours = range(3)

    def region(k, phase, s, i, h):
        order = orders[k]
        index = []
        for name in 'zyx':
            if name == order[phase]:
                index.append((where[name] + i) % SIDE)
            elif phase and name == order[phase - 1]:
                index.append((where[name] + shifts[s]) % SIDE)
            elif name in order[:phase]:
                index.append(slice(None))
            else:
                index.append(where[name])
        return out_ref.at[(*index, pl.ds(h * (n_rows // 2), n_rows // 2), pl.ds(k * third, third))]

    def owned(k, h):
        return own.at[pl.ds(h * (n_rows // 2), n_rows // 2), pl.ds(k * third, third)]

    def issue(phase, s):
        copies = []
        for turn in range(2):
            for k in colours:
                dim = orders[k][phase]
                base = 54 * k + 24 * max(phase - 1, 0) + 6 * (phase > 0) + 6 * s + 2 * turn
                for way, target in ((0, ups[dim]), (1, downs[dim])):
                    h = way if turn == 0 else 1 - way
                    src = owned(k, h) if phase == 0 or (phase == 1 and s == 0) else region(k, phase, s, 0, h)
                    copies.append((k, turn, way, push(src, region(k, phase, s, 0, h), sems_ag, base + way, target)))
        started.extend(copy for _, _, _, copy in copies)
        return {(k, turn, way): copy for k, turn, way, copy in copies}

    def relay(phase, s, sent):
        passed = {}
        for k in colours:
            dim = orders[k][phase]
            base = 54 * k + 24 * max(phase - 1, 0) + 6 * (phase > 0) + 6 * s + 4
            for way, target in ((0, ups[dim]), (1, downs[dim])):
                sent[k, 0, way].wait_recv()
                spot = region(k, phase, s, 1 if way else 3, way)
                passed[k, way] = push(spot, spot, sems_ag, base + way, target)
        started.extend(passed.values())
        return passed

    def settle(sent_sets, way):
        for sent in sent_sets:
            for k in colours:
                sent[k, 1, way].wait_recv()

    sent = {0: [issue(0, 0)], 1: [issue(1, 0)], 2: []}
    for phase in range(3):
        passed = [relay(phase, s, some) for s, some in enumerate(sent[phase])]
        for way in range(2):
            settle(sent[phase], way)
            if phase < 2:
                sent[phase + 1].append(issue(phase + 1, way + 1))
        for some in passed:
            for copy in some.values():
                copy.wait_recv()
        if phase < 2:
            sent[phase + 1].append(issue(phase + 1, 3))
        if phase == 0:
            keep.wait()
            sent[2].append(issue(2, 0))
    for copy in started:
        copy.wait_send()


def moe(hid, ids, gate_wts, pos, spread, weights):
    blocks, n_rows, depth = hid.shape
    width = depth // 2
    rows = weights.shape[1] // 2
    f32, bf16 = jnp.float32, jnp.bfloat16
    dma = pltpu.SemaphoreType.DMA
    return pl.pallas_call(
        moe_kernel,
        out_shape=jax.ShapeDtypeStruct((SIDE, SIDE, SIDE, n_rows, depth), bf16),
        in_specs=[pl.BlockSpec(memory_space=pl.ANY)] + [pl.BlockSpec(memory_space=pltpu.VMEM)] * 5,
        out_specs=pl.BlockSpec(memory_space=pl.ANY),
        scratch_shapes=[
            pltpu.VMEM((SIDE * SIDE, n_rows, depth), bf16),
            pltpu.VMEM((spread.shape[0], ids.shape[1]), f32),
            pltpu.VMEM((SIDE * SIDE, n_rows, spread.shape[1]), f32),
            pltpu.VMEM((SIDE, 3, 2, 2, rows, depth), bf16),
            pltpu.VMEM((2, len(PLACES), n_rows, width), f32),
            pltpu.VMEM((2, 2, SIDE, n_rows // 2, width), f32),
            pltpu.VMEM((2, 2, SIDE, n_rows, width), f32),
            pltpu.VMEM((2, SIDE, n_rows, width), f32),
            pltpu.VMEM((2, 2, n_rows // 2, width), f32),
            pltpu.VMEM((2, 2, n_rows, width), f32),
            pltpu.VMEM((n_rows, depth), bf16),
            dma((16,)), dma, dma((12,)), dma((12,)), dma((14,)), dma((14,)), dma((60,)), dma((60,)), dma((162,)), dma((162,)),
        ],
        compiler_params=pltpu.CompilerParams(collective_id=0, has_side_effects=True, vmem_limit_bytes=38 * 2 ** 20),
        name='moe',
    )(hid, ids, gate_wts, pos, spread, weights)


def solution(mesh):
    row_spec = P(('dp', 'ep'), None)
    col_spec = P('ep', None, 'etp')
    in_specs = (row_spec, row_spec, row_spec, row_spec, col_spec, col_spec, P('ep', 'etp', None))

    def device_step(hidden, expert_ids, gate_wts, slot_pos, w_gate, w_up, w_down):
        rows, d_model = hidden.shape
        local_experts, _, width = w_gate.shape
        experts = 2 * local_experts
        chips = SIDE ** 3
        block = rows // chips

        local = [w.transpose(0, 2, 1) for w in (w_gate, w_up)] + [w_down]
        local = jnp.stack([w.reshape(local_experts * width, d_model) for w in local])

        cols = experts * width
        per_term = experts + 8
        dim, core, expert, _ = np.unravel_index(np.arange(cols), (2, 2, local_experts // 2, width))
        spread = np.zeros((3 * per_term, -(-(cols + 1) // 128) * 128), np.float32)
        for n in range(3):
            spread[n * per_term + core * local_experts + dim * (local_experts // 2) + expert, np.arange(cols)] = 1
            spread[n * per_term + experts, cols] = 1
        out = moe(hidden.reshape(chips, block, d_model), expert_ids.T, gate_wts.T, slot_pos.T,
                  jnp.asarray(spread, jnp.bfloat16), local)
        return out.reshape(rows, d_model)

    return jax.shard_map(device_step, mesh=mesh, in_specs=in_specs, out_specs=row_spec, check_vma=False)
```
